32 devices in a mesh: grp: 4 (over y, x), row: 8 (over z, core).
Axes of the slice: x: 2, y: 2, z: 4, core: 2. Of those that a mesh axis runs over, the one named last changes fastest.
Arguments:
- owned_blocks: int32 [1024], P(('grp', 'row')), may hold values from 0 to 1023, as said below
- live_count: int32 [32], P(('grp', 'row')), may hold values from 9 to 36, as said below
- row_block: int32 [1152], P(('grp', 'row')), may hold values from 0 to 1023, as said below
- column_block: int32 [1152], P(('grp', 'row')), may hold values from 0 to 1023, as said below
- send_list: int32 [4, 8, 4, 24], P('grp', 'row'), may hold values from -1 to 31, as said below
- receive_list: int32 [4, 8, 4, 24], P('grp', 'row'), may hold values from -1 to 1023, as said below
- block_values: bfloat16 [1152, 256, 256], P(('grp', 'row')), as said below
- node_shift: float32 [1024, 256], P(('grp', 'row')), may hold values from 0.1 to 2
- start_vector: float32 [1024, 256], P(('grp', 'row')), as said below
Outputs:
- lanczos_basis: float32 [17, 1024, 256], P(None, ('grp', 'row'))
- tridiagonal: float32 [2, 16], replicated
The draws below stay inside these ranges and needn't reach their ends.
Inputs may be any that keep to these rules, and one draw needn't show every extreme that they name: `owned_blocks`: A permutation of the block ids 0 to 1023. `live_count`: some device has exactly 36 live slots in every draw. `row_block`: every slot's row block is owned by the slot's device. `column_block`: every slot's column block is owned by the slot's device or appears in that device's receive_list. Nonempty entries come first in each list and are distinct; a device sends nothing to itself; send_list[p, r, g] names exactly the blocks whose ids receive_list[g, r, p] lists, in the same order. Some list is full in every draw, and some device receives a full list from every peer. `receive_list`: matches send_list as stated there. `block_values`: entries are finite and of moderate size. `start_vector`: entries are finite and of order one.
All inputs are finite; a program needn't handle non-finite values.
Results may differ from the reference program's by a relative error of at most 0.0034.
Values may be sent and summed in bfloat16 or wider, within the bound.
No kernel may reach another device: no remote copies, remote signals or barrier semaphores. Data moves between devices by JAX's collectives and lax.ppermute only.
A program may use at most 64 MiB of HBM per device.

```python
import math
import jax
import jax.numpy as jnp
from jax import lax

BLOCK = 256
BLOCKS_DEV = 32
STEPS = 16
SLOTS_DEV = 36
HALO = 24
BLOCKS = 1024
SLOTS = 1152
N_GRP = 4
N_ROW = 8


def layout(key):
    base = jax.random.fold_in(key, 9173)
    groups = N_GRP
    row_ranks = N_ROW
    devices_all = groups * row_ranks
    own_keys = jax.random.split(jax.random.fold_in(base, 1), row_ranks)
    shuffled = jax.vmap(lambda one_key: jax.random.permutation(one_key, groups * BLOCKS_DEV))(own_keys).astype(jnp.int32)
    owned_ids = jnp.arange(row_ranks, dtype=jnp.int32)[:, None] * (groups * BLOCKS_DEV) + shuffled
    owned_ids = owned_ids.reshape(row_ranks, groups, BLOCKS_DEV).transpose(1, 0, 2)
    sent_count = jax.random.randint(jax.random.fold_in(base, 2), (groups, groups, row_ranks), HALO // 4, HALO + 1)
    offset_peer = jax.random.randint(jax.random.fold_in(base, 3), (), 1, groups)
    sender_idx = jnp.arange(groups)[:, None, None]
    receiver_idx = jnp.arange(groups)[None, :, None]
    rank_idx = jnp.arange(row_ranks)[None, None, :]
    sent_count = jnp.where(sender_idx == (receiver_idx + offset_peer) % groups, HALO, sent_count)
    full_group = jax.random.randint(jax.random.fold_in(base, 4), (), 0, groups)
    full_rank = jax.random.randint(jax.random.fold_in(base, 5), (), 0, row_ranks)
    sent_count = jnp.where((receiver_idx == full_group) & (rank_idx == full_rank), HALO, sent_count)
    sent_count = jnp.where(sender_idx == receiver_idx, 0, sent_count)
    pick_keys = jax.random.split(jax.random.fold_in(base, 6), groups * groups * row_ranks)
    chosen = jax.vmap(lambda one_key: jax.random.permutation(one_key, BLOCKS_DEV))(pick_keys)
    chosen = chosen.reshape(groups, groups, row_ranks, BLOCKS_DEV)[..., :HALO].astype(jnp.int32)
    valid = jnp.arange(HALO)[None, None, None, :] < sent_count[..., None]
    send_full = jnp.where(valid, chosen, -1)
    owner_rows = jnp.broadcast_to(owned_ids[:, None, :, :], (groups, groups, row_ranks, BLOCKS_DEV))
    sent_ids = jnp.where(valid, jnp.take_along_axis(owner_rows, chosen, axis=3), -1)
    send_list = send_full.transpose(0, 2, 1, 3).astype(jnp.int32)
    receive_list = sent_ids.transpose(1, 2, 0, 3).astype(jnp.int32)
    owned_flat = owned_ids.reshape(devices_all, BLOCKS_DEV)
    spread = jax.random.randint(jax.random.fold_in(base, 7), (devices_all,), 0, 49)
    counts = jnp.maximum(SLOTS_DEV // 4, SLOTS_DEV * 16 // (16 + spread))
    busiest = jax.random.randint(jax.random.fold_in(base, 8), (), 0, devices_all)
    counts = jnp.where(jnp.arange(devices_all) == busiest, SLOTS_DEV, counts).astype(jnp.int32)
    first_rows = jax.vmap(lambda one_key: jax.random.permutation(one_key, BLOCKS_DEV))(jax.random.split(jax.random.fold_in(base, 9), devices_all))
    extra_rows = jax.random.randint(jax.random.fold_in(base, 10), (devices_all, SLOTS_DEV - BLOCKS_DEV), 0, BLOCKS_DEV)
    local_rows = jnp.concatenate([first_rows.astype(jnp.int32), extra_rows.astype(jnp.int32)], axis=1)
    row_ids = jnp.take_along_axis(owned_flat, local_rows, axis=1)
    pool = jnp.concatenate([owned_flat, receive_list.reshape(devices_all, groups * HALO)], axis=1)
    drawn = jax.random.randint(jax.random.fold_in(base, 11), (devices_all, SLOTS_DEV), 0, BLOCKS_DEV + groups * HALO)
    picked = jnp.take_along_axis(pool, drawn, axis=1)
    fallback = jnp.take_along_axis(owned_flat, drawn % BLOCKS_DEV, axis=1)
    column_ids = jnp.where(picked < 0, fallback, picked).astype(jnp.int32)
    return (owned_flat.reshape(-1), counts, row_ids.reshape(-1).astype(jnp.int32), column_ids.reshape(-1), send_list, receive_list)


def draw_owned_blocks(key, part):
    return layout(key)[0]


def draw_live_count(key, part):
    return layout(key)[1]


def draw_row_block(key, part):
    return layout(key)[2]


def draw_column_block(key, part):
    return layout(key)[3]


def draw_send_list(key, part):
    return layout(key)[4]


def draw_receive_list(key, part):
    return layout(key)[5]


def draw_block_values(key, part):
    device = (jnp.arange(SLOTS) // SLOTS_DEV).astype(jnp.float32)
    rising = 1.0 + 2.0 * device / max(N_GRP * N_ROW - 1, 1)
    samples = jax.random.normal(key, (SLOTS, BLOCK, BLOCK), jnp.float32)
    return (samples * (rising / BLOCK ** 0.5)[:, None, None]).astype(jnp.bfloat16)


def draw_start_vector(key, part):
    device = (jnp.arange(BLOCKS) // BLOCKS_DEV).astype(jnp.float32)
    rising = 1.0 + 2.0 * device / max(N_GRP * N_ROW - 1, 1)
    samples = jax.random.normal(key, (BLOCKS, BLOCK), jnp.float32)
    return (samples * rising[:, None]).astype(jnp.float32)


def steps_of(own_key, extent, cuts, least, top_value):
    def one(axis_at, blocks):
        draws = jax.random.uniform(jax.random.fold_in(jax.random.fold_in(own_key, 6), axis_at), (blocks,), jnp.float32, least / len(cuts), top_value / len(cuts))
        return jnp.repeat(jnp.exp(draws), extent[axis_at] // blocks).reshape((-1,) + (1,) * (len(extent) - axis_at - 1))

    loudness = one(*cuts[0])
    for cut in cuts[1:]:
        loudness = loudness * one(*cut)
    return loudness


def setup_inputs(seed: int = 0) -> dict:
    key_of = jax.random.split(jax.random.key(seed), 10)
    return {
        "owned_blocks": draw_owned_blocks(jax.random.fold_in(key_of[9], 71), 0),
        "live_count": draw_live_count(jax.random.fold_in(key_of[9], 71), 0),
        "row_block": draw_row_block(jax.random.fold_in(key_of[9], 71), 0),
        "column_block": draw_column_block(jax.random.fold_in(key_of[9], 71), 0),
        "send_list": draw_send_list(jax.random.fold_in(key_of[9], 71), 0),
        "receive_list": draw_receive_list(jax.random.fold_in(key_of[9], 71), 0),
        "block_values": draw_block_values(jax.random.fold_in(key_of[9], 71), 0),
        "node_shift": jnp.clip(jnp.exp(math.log(2.0) - 2.9957323 * jax.random.uniform(key_of[7], (BLOCKS, BLOCK), jnp.float32) ** steps_of(key_of[7], (BLOCKS, BLOCK), ((0, 32),), -0.2, 0.2)), 0.1, 2.0),
        "start_vector": draw_start_vector(jax.random.fold_in(key_of[9], 71), 0),
    }


def reference(owned_blocks, live_count, row_block, column_block, send_list, receive_list, block_values, node_shift, start_vector):
    groups = N_GRP
    row_ranks = N_ROW
    devices_all = groups * row_ranks
    owned_rows = owned_blocks.reshape(devices_all, BLOCKS_DEV)
    peer_base = (jnp.arange(groups, dtype=jnp.int32)[None, None, :, None] * row_ranks + jnp.arange(row_ranks, dtype=jnp.int32)[None, :, None, None]) * BLOCKS_DEV
    source_send = jnp.transpose(send_list, (2, 1, 0, 3))
    source_pos = (peer_base + jnp.clip(source_send, 0, BLOCKS_DEV - 1)).astype(jnp.int32).reshape(devices_all, groups * HALO)
    own_pos = jnp.arange(devices_all * BLOCKS_DEV, dtype=jnp.int32).reshape(devices_all, BLOCKS_DEV)
    known_ids = jnp.concatenate([owned_rows, receive_list.reshape(devices_all, groups * HALO)], axis=1)
    known_pos = jnp.concatenate([own_pos, source_pos], axis=1)
    columns_dev = column_block.reshape(devices_all, SLOTS_DEV)
    column_match = columns_dev[:, :, None] == known_ids[:, None, :]
    column_index = jnp.argmax(column_match.astype(jnp.int32), axis=2).astype(jnp.int32)
    column_pos = jnp.take_along_axis(known_pos, column_index, axis=1).reshape(-1)
    rows_dev = row_block.reshape(devices_all, SLOTS_DEV)
    row_match = rows_dev[:, :, None] == owned_rows[:, None, :]
    row_local = jnp.argmax(row_match.astype(jnp.int32), axis=2).astype(jnp.int32)
    row_pos = (own_pos[:, :1] + row_local).reshape(-1)
    keep_slot = jnp.arange(SLOTS_DEV, dtype=jnp.int32)[None, :] < live_count[:, None]
    weight = keep_slot.astype(jnp.float32).reshape(-1, 1)
    values_dev = block_values.reshape(devices_all, SLOTS_DEV, BLOCK, BLOCK)
    row_sums = lax.map(lambda part: lax.optimization_barrier(jnp.sum(part.astype(jnp.float32), axis=2)), values_dev).reshape(-1, BLOCK)
    degree = jax.ops.segment_sum(row_sums * weight, row_pos, num_segments=BLOCKS)
    diagonal = degree + node_shift

    def apply_operator(vector):
        rounded = vector.astype(jnp.bfloat16)
        gathered = rounded[column_pos].reshape(devices_all, SLOTS_DEV, BLOCK)
        products = lax.map(lambda pair: jnp.einsum('sab,sb->sa', pair[0].astype(jnp.float32), pair[1].astype(jnp.float32)), (values_dev, gathered)).reshape(-1, BLOCK)
        coupling = jax.ops.segment_sum(products * weight, row_pos, num_segments=BLOCKS)
        return diagonal * vector - coupling
    entries = BLOCKS * BLOCK
    highest = lax.Precision.HIGHEST
    first_vector = start_vector * lax.rsqrt(jnp.sum(start_vector * start_vector) / entries + 1e-06)
    krylov = jnp.zeros((STEPS + 1, BLOCKS, BLOCK), jnp.float32).at[0].set(first_vector)
    alphas = []
    betas = []
    for step_index in range(STEPS):
        applied = apply_operator(krylov[step_index])
        coefficient = jnp.einsum('kpb,pb->k', krylov, applied, precision=highest) / entries
        projected = applied - jnp.einsum('k,kpb->pb', coefficient, krylov, precision=highest)
        square_mean = jnp.sum(projected * projected) / entries
        alphas.append(coefficient[step_index])
        betas.append(jnp.sqrt(square_mean))
        krylov = krylov.at[step_index + 1].set(projected * lax.rsqrt(square_mean + 1e-06))
    tridiagonal = jnp.stack([jnp.stack(alphas), jnp.stack(betas)])
    return (krylov, tridiagonal)
```

```python
import functools

import jax
import jax.numpy as jnp
from jax import lax
from jax.experimental import pallas as pl
from jax.experimental.pallas import tpu as pltpu
from jax.sharding import PartitionSpec as P

STEPS = 16
SQUARE = STEPS
LANES = 128
AXES = ("grp", "row")
VMEM = pltpu.MemorySpace.VMEM
SMEM = pltpu.MemorySpace.SMEM


def spec(space=VMEM):
    return pl.BlockSpec(memory_space=space)


def call(kernel, outs, operands, spaces=None, scratch=(), flops=0):
    many = isinstance(outs, (tuple, list))
    return pl.pallas_call(
        kernel,
        out_shape=outs,
        in_specs=[spec(s) for s in (spaces or [VMEM] * len(operands))],
        out_specs=[spec()] * len(outs) if many else spec(),
        scratch_shapes=list(scratch),
        compiler_params=pltpu.CompilerParams(vmem_limit_bytes=24 << 20),
        cost_estimate=pl.CostEstimate(flops=flops, bytes_accessed=1 << 16, transcendentals=0),
    )(*operands)


def fold(x):
    half = x.shape[1] // 2
    x = x[:, :half] + x[:, half:]
    total = x[0:8]
    for i in range(8, x.shape[0], 8):
        total = total + x[i : i + 8]
    return jnp.sum(total, axis=0, keepdims=True)


def emit_partials(rows_ref, out_ref):
    total = jnp.sum(rows_ref[...], axis=1, keepdims=True)
    place = lax.broadcasted_iota(jnp.int32, rows_ref.shape, 0)
    lane = lax.broadcasted_iota(jnp.int32, rows_ref.shape, 1)
    row = jnp.sum(jnp.where(lane == place, total, 0.0), axis=0, keepdims=True)
    out_ref[...] = jnp.broadcast_to(row, out_ref.shape)


def read_sums(gathered_ref, scale):
    total = jnp.sum(gathered_ref[...], axis=0, keepdims=True) * scale
    place = lax.broadcasted_iota(jnp.int32, (24, LANES), 0)
    lane = lax.broadcasted_iota(jnp.int32, (24, LANES), 1)
    return jnp.sum(jnp.where(lane == place, total, 0.0), axis=1, keepdims=True)


def init_kernel(start_ref, ids_ref, out_ref, spread_ref, rows_ref):
    rows, width = start_ref.shape
    start = start_ref[...]
    out_ref[0:rows, :] = start
    out_ref[rows : rows + 8, :] = jnp.zeros((8, width), jnp.float32)
    out_ref[rows : rows + 1, 0:rows] = ids_ref[...].astype(jnp.float32)
    rows_ref[...] = jnp.zeros_like(rows_ref)
    rows_ref[SQUARE : SQUARE + 1, :] = fold(start * start)
    emit_partials(rows_ref, spread_ref)


def transpose_kernel(source_ref, out_ref):
    for s in range(source_ref.shape[0]):
        out_ref[s] = source_ref[s].T


def coefficients(j, gathered_ref, scale):
    means = read_sums(gathered_ref, scale)
    square = means[SQUARE : SQUARE + 1, :]
    if j:
        used = means[0:j, :]
        square = jnp.maximum(square - jnp.sum(used * used, axis=0, keepdims=True), 0.0)
    return means, square, lax.rsqrt(square + 1e-6)


def record(j, means, square, tri):
    lane = lax.broadcasted_iota(jnp.int32, tri.shape, 1)
    place = lax.broadcasted_iota(jnp.int32, tri.shape, 0)
    column = jnp.where(place == 0, means[j - 1 : j, :], jnp.sqrt(square))
    return jnp.where(lane == j - 1, column, tri)


def step_kernel(j, peers, scale, *refs):
    parts = refs[:peers]
    gathered_ref = refs[peers]
    basis = refs[peers + 1 : peers + 1 + j]
    blocks_ref, index_ref, diag_ref, tri_ref = refs[peers + 1 + j : peers + 5 + j]
    vector_ref, out_ref, spread_ref, tri_out, *more = refs[peers + 5 + j :]
    if j == 0:
        diag_out, acc_ref, rows_ref = more
    else:
        acc_ref, rows_ref = more
    slots = blocks_ref.shape[0]
    rows, width = diag_ref.shape
    halves = width // LANES

    means, square, inverse = coefficients(j, gathered_ref, scale)
    tri = tri_ref[...]
    tri_out[...] = record(j, means, square, tri) if j else tri
    for p in range(peers):
        value = parts[p][0:rows, :]
        for k in range(j):
            value = value - means[k : k + 1, :] * basis[k][rows * p : rows * (p + 1), :]
        vector_ref[rows * p : rows * (p + 1), :] = value * inverse

    acc_ref[...] = jnp.zeros_like(acc_ref)
    sub = lax.broadcasted_iota(jnp.int32, (8, width), 0)
    fill = jnp.where(sub == 1, 1.0, 0.0) if j == 0 else jnp.zeros((8, width), jnp.float32)
    for s in range(slots):
        vector = jnp.broadcast_to(vector_ref[pl.ds(index_ref[0, s], 1), :], (8, width))
        left = jnp.where(sub == 0, vector, fill).astype(jnp.bfloat16)
        product = jnp.dot(left, blocks_ref[s], preferred_element_type=jnp.float32)
        target = pl.ds(pl.multiple_of(index_ref[1, s] * 8, 8), 8)
        for h in range(halves):
            acc_ref[h, target, :] = acc_ref[h, target, :] + product[:, LANES * h : LANES * (h + 1)]

    def gather(i):
        found = [acc_ref.at[h][pl.ds(i, rows, stride=8), :] for h in range(halves)]
        return jnp.concatenate(found, axis=1)

    diagonal = diag_ref[...]
    if j == 0:
        diagonal = diagonal + gather(1)
        diag_out[...] = diagonal
    image = diagonal * vector_ref[0:rows, :] - gather(0)
    out_ref[...] = image
    rows_ref[...] = jnp.zeros_like(rows_ref)
    for k in range(j + 1):
        own = vector_ref[0:rows, :] if k == j else basis[k][0:rows, :]
        rows_ref[k : k + 1, :] = fold(own * image)
    rows_ref[SQUARE : SQUARE + 1, :] = fold(image * image)
    emit_partials(rows_ref, spread_ref)


def finish_kernel(scale, image_ref, gathered_ref, *refs):
    basis = refs[:STEPS]
    tri_ref, out_ref, tri_out = refs[STEPS:]
    rows = image_ref.shape[0]
    means, square, inverse = coefficients(STEPS, gathered_ref, scale)
    tri_out[...] = record(STEPS, means, square, tri_ref[...])[0:2, 0:STEPS]
    value = image_ref[...]
    for k in range(STEPS):
        own = basis[k][0:rows, :]
        out_ref[k] = own
        value = value - means[k : k + 1, :] * own
    out_ref[STEPS] = value * inverse


def shards(
    owned_blocks,
    live_count,
    row_block,
    column_block,
    send_list,
    receive_list,
    block_values,
    node_shift,
    start_vector,
):
    rows, width = start_vector.shape
    slots = block_values.shape[0]
    groups = lax.axis_size("grp")
    devices = groups * lax.axis_size("row")
    scale = 1.0 / float(devices * rows * width)
    f32 = jnp.float32

    def exchange(payload):
        parts = [payload]
        for k in range(groups - 1, 0, -1):
            if groups & (groups - 1):
                pairs = [(i, (i + k) % groups) for i in range(groups)]
            else:
                pairs = [(i, i ^ k) for i in range(groups)]
            parts.insert(1, lax.ppermute(payload, "grp", pairs))
        return parts

    def spread_out(spread):
        rows_out = lax.all_to_all(
            spread.reshape(devices, 1, LANES), AXES, split_axis=0, concat_axis=0, tiled=True
        )
        return rows_out.reshape(devices, LANES)

    spread_shape = jax.ShapeDtypeStruct((devices, LANES), f32)
    rows_scratch = pltpu.VMEM((24, LANES), f32)
    payload, spread = call(
        init_kernel,
        [jax.ShapeDtypeStruct((rows + 8, width), f32), spread_shape],
        [start_vector, owned_blocks.reshape(1, rows)],
        None,
        [rows_scratch],
    )
    gathered = spread_out(spread)
    parts = exchange(payload)
    blocks = call(
        transpose_kernel,
        jax.ShapeDtypeStruct(block_values.shape, block_values.dtype),
        [block_values],
        flops=1 << 20,
    )
    known = jnp.concatenate([part[rows, :rows] for part in parts])
    match = column_block.astype(f32)[:, None] == known[None, :]
    column = jnp.argmax(match.astype(jnp.int32), axis=1).astype(jnp.int32)
    row_match = row_block[:, None] == owned_blocks[None, :]
    target = jnp.argmax(row_match.astype(jnp.int32), axis=1).astype(jnp.int32)
    live = jnp.arange(slots, dtype=jnp.int32) < live_count[0]
    target = jnp.where(live, target, rows)
    index = jnp.stack([column, target])

    diagonal = node_shift
    tri = jnp.zeros((8, LANES), f32)
    basis = []
    for j in range(STEPS):
        outs = [
            jax.ShapeDtypeStruct((groups * rows, width), f32),
            jax.ShapeDtypeStruct((rows, width), f32),
            spread_shape,
            jax.ShapeDtypeStruct((8, LANES), f32),
        ]
        if j == 0:
            outs.append(jax.ShapeDtypeStruct((rows, width), f32))
        result = call(
            functools.partial(step_kernel, j, groups, scale),
            outs,
            [*parts, gathered, *basis, blocks, index, diagonal, tri],
            [VMEM] * (groups + j + 2) + [SMEM, VMEM, VMEM],
            [pltpu.VMEM((width // LANES, (rows + 1) * 8, LANES), f32), rows_scratch],
            flops=2 * slots * width * width * 8,
        )
        if j == 0:
            diagonal = result[4]
        basis.append(result[0])
        image, spread, tri = result[1:4]
        gathered = spread_out(spread)
        if j < STEPS - 1:
            parts = exchange(image)
    return call(
        functools.partial(finish_kernel, scale),
        [
            jax.ShapeDtypeStruct((STEPS + 1, rows, width), f32),
            jax.ShapeDtypeStruct((2, STEPS), f32),
        ],
        [image, gathered, *basis, tri],
    )


def solution(mesh):
    return jax.shard_map(
        shards,
        mesh=mesh,
        in_specs=(
            P(("grp", "row")),
            P(("grp", "row")),
            P(("grp", "row")),
            P(("grp", "row")),
            P("grp", "row", None, None),
            P("grp", "row", None, None),
            P(("grp", "row"), None, None),
            P(("grp", "row"), None),
            P(("grp", "row"), None),
        ),
        out_specs=(P(None, ("grp", "row"), None), P()),
        check_vma=False,
    )
```

```python
import functools

import jax
import jax.numpy as jnp
from jax import lax
from jax.experimental import pallas as pl
from jax.experimental.pallas import tpu as pltpu
from jax.sharding import PartitionSpec as P

STEPS = 16
SQUARE = STEPS
LANES = 128
FULL = 67_000_000 // 1024 * 1024
AXES = ("grp", "row")
VMEM = pltpu.MemorySpace.VMEM
HBM = pltpu.MemorySpace.HBM


def spec(space=VMEM):
    return pl.BlockSpec(memory_space=space)


def call(kernel, outs, operands, spaces=None, scratch=(), flops=0, limit=24 << 20):
    many = isinstance(outs, (tuple, list))
    return pl.pallas_call(
        kernel,
        out_shape=outs,
        in_specs=[spec(s) for s in (spaces or [VMEM] * len(operands))],
        out_specs=[spec()] * len(outs) if many else spec(),
        scratch_shapes=list(scratch),
        compiler_params=pltpu.CompilerParams(vmem_limit_bytes=limit),
        cost_estimate=pl.CostEstimate(flops=flops, bytes_accessed=1 << 16, transcendentals=0),
    )(*operands)


def fold(x):
    half = x.shape[1] // 2
    x = x[:, :half] + x[:, half:]
    total = x[0:8]
    for i in range(8, x.shape[0], 8):
        total = total + x[i : i + 8]
    return jnp.sum(total, axis=0, keepdims=True)


def emit_partials(rows_ref, out_ref):
    total = jnp.sum(rows_ref[...], axis=1, keepdims=True)
    place = lax.broadcasted_iota(jnp.int32, rows_ref.shape, 0)
    lane = lax.broadcasted_iota(jnp.int32, rows_ref.shape, 1)
    row = jnp.sum(jnp.where(lane == place, total, 0.0), axis=0, keepdims=True)
    out_ref[...] = jnp.broadcast_to(row, out_ref.shape)


def read_sums(gathered_ref, scale):
    total = jnp.sum(gathered_ref[...], axis=0, keepdims=True) * scale
    place = lax.broadcasted_iota(jnp.int32, (24, LANES), 0)
    lane = lax.broadcasted_iota(jnp.int32, (24, LANES), 1)
    return jnp.sum(jnp.where(lane == place, total, 0.0), axis=1, keepdims=True)


def column_of(row, count):
    place = lax.broadcasted_iota(jnp.int32, (count, row.shape[1]), 0)
    lane = lax.broadcasted_iota(jnp.int32, (count, row.shape[1]), 1)
    return jnp.sum(jnp.where(place == lane, row, 0), axis=1, keepdims=True)


def place_of(wanted, known, offset):
    place = lax.broadcasted_iota(jnp.int32, (known.shape[0], wanted.shape[1]), 0) + offset
    return jnp.sum(jnp.where(known == wanted, place, 0), axis=0, keepdims=True)


def init_kernel(
    start_hbm, ids_hbm, wanted_hbm, column_hbm, live_hbm, out_ref, index_ref,
    start_ref, ids_ref, wanted_ref, column_ref, live_ref, sems,
):
    pairs = [
        (start_hbm, start_ref),
        (ids_hbm, ids_ref),
        (wanted_hbm, wanted_ref),
        (column_hbm, column_ref),
        (live_hbm, live_ref),
    ]
    copies = [pltpu.make_async_copy(x, y, sems.at[i]) for i, (x, y) in enumerate(pairs)]
    for copy in copies:
        copy.start()
    for copy in copies:
        copy.wait()
    rows, width = start_ref.shape
    start = start_ref[...]
    ids = ids_ref[...]
    out_ref[0:rows, :] = start
    out_ref[rows : rows + 8, :] = jnp.zeros((8, width), jnp.float32)
    out_ref[rows : rows + 1, 0:rows] = ids.astype(jnp.float32)
    found = place_of(wanted_ref[...], column_of(ids, rows), 0)
    lane = lax.broadcasted_iota(jnp.int32, found.shape, 1)
    target = jnp.where(lane < live_ref[...], found, rows)
    index_ref[...] = jnp.concatenate([column_ref[...], target], axis=0)


def find_columns(parts, wanted):
    rows = parts[0].shape[0] - 8
    column = jnp.zeros(wanted.shape, jnp.int32)
    for p, part in enumerate(parts):
        ids = part[rows : rows + 1, 0:rows].astype(jnp.int32)
        column = column + place_of(wanted, column_of(ids, rows), rows * p)
    return column


def setup_kernel(source_hbm, payload_ref, out_ref, spread_ref, buffer_ref, rows_ref, sems):
    slots = source_hbm.shape[0]
    chunk = -(-slots // sems.shape[0])
    chunks = [pl.ds(s, min(chunk, slots - s)) for s in range(0, slots, chunk)]
    copies = [
        pltpu.make_async_copy(source_hbm.at[part], buffer_ref.at[part], sems.at[i])
        for i, part in enumerate(chunks)
    ]
    for copy in copies:
        copy.start()
    start = payload_ref[0 : payload_ref.shape[0] - 8, :]
    rows_ref[...] = jnp.zeros_like(rows_ref)
    rows_ref[SQUARE : SQUARE + 1, :] = fold(start * start)
    emit_partials(rows_ref, spread_ref)
    for part, copy in zip(chunks, copies):
        copy.wait()
        for s in range(part.start, part.start + part.size):
            out_ref[s] = buffer_ref[s].T


def coefficients(j, gathered_ref, scale):
    means = read_sums(gathered_ref, scale)
    square = means[SQUARE : SQUARE + 1, :]
    if j:
        used = means[0:j, :]
        square = jnp.maximum(square - jnp.sum(used * used, axis=0, keepdims=True), 0.0)
    return means, square, lax.rsqrt(square + 1e-6)


def record(j, means, square, tri):
    lane = lax.broadcasted_iota(jnp.int32, tri.shape, 1)
    place = lax.broadcasted_iota(jnp.int32, tri.shape, 0)
    column = jnp.where(place == 0, means[j - 1 : j, :], jnp.sqrt(square))
    return jnp.where(lane == j - 1, column, tri)


def step_kernel(j, peers, scale, *refs):
    parts = refs[:peers]
    gathered_ref = refs[peers]
    basis = refs[peers + 1 : peers + 1 + j]
    blocks_ref, index_ref, diag_ref, tri_ref = refs[peers + 1 + j : peers + 5 + j]
    if j == 0:
        vector_ref, out_ref, spread_ref, tri_out, diag_out, index_out = refs[peers + 5 :][:6]
        given, index_ref = index_ref[...], index_out
        index_ref[...] = jnp.concatenate([find_columns(parts, given[0:1]), given[1:2]], axis=0)
    else:
        vector_ref, out_ref, spread_ref, tri_out = refs[peers + 5 + j :][:4]
    acc_ref, rows_ref, table_ref, sem = refs[-4:]
    table = pltpu.make_async_copy(index_ref, table_ref, sem)
    table.start()
    slots = blocks_ref.shape[0]
    rows, width = diag_ref.shape
    halves = width // LANES

    means, square, inverse = coefficients(j, gathered_ref, scale)
    tri = tri_ref[...]
    tri_out[...] = record(j, means, square, tri) if j else tri
    for p in range(peers):
        value = parts[p][0:rows, :]
        for k in range(j):
            value = value - means[k : k + 1, :] * basis[k][rows * p : rows * (p + 1), :]
        vector_ref[rows * p : rows * (p + 1), :] = value * inverse

    acc_ref[...] = jnp.zeros_like(acc_ref)
    sub = lax.broadcasted_iota(jnp.int32, (8, width), 0)
    table.wait()
    fill = jnp.where(sub == 1, 1.0, 0.0) if j == 0 else jnp.zeros((8, width), jnp.float32)
    for s in range(slots):
        vector = jnp.broadcast_to(vector_ref[pl.ds(table_ref[0, s], 1), :], (8, width))
        left = jnp.where(sub == 0, vector, fill).astype(jnp.bfloat16)
        product = jnp.dot(left, blocks_ref[s], preferred_element_type=jnp.float32)
        target = pl.ds(pl.multiple_of(table_ref[1, s] * 8, 8), 8)
        for h in range(halves):
            acc_ref[h, target, :] = acc_ref[h, target, :] + product[:, LANES * h : LANES * (h + 1)]

    def gather(i):
        found = [acc_ref.at[h][pl.ds(i, rows, stride=8), :] for h in range(halves)]
        return jnp.concatenate(found, axis=1)

    diagonal = diag_ref[...]
    if j == 0:
        diagonal = diagonal + gather(1)
        diag_out[...] = diagonal
    image = diagonal * vector_ref[0:rows, :] - gather(0)
    out_ref[...] = image
    rows_ref[...] = jnp.zeros_like(rows_ref)
    for k in range(j + 1):
        own = vector_ref[0:rows, :] if k == j else basis[k][0:rows, :]
        rows_ref[k : k + 1, :] = fold(own * image)
    rows_ref[SQUARE : SQUARE + 1, :] = fold(image * image)
    emit_partials(rows_ref, spread_ref)


def finish_kernel(scale, image_ref, gathered_ref, *refs):
    basis = refs[:STEPS]
    tri_ref, out_ref, tri_out = refs[STEPS:]
    rows = image_ref.shape[0]
    means, square, inverse = coefficients(STEPS, gathered_ref, scale)
    tri_out[...] = record(STEPS, means, square, tri_ref[...])[0:2, 0:STEPS]
    value = image_ref[...]
    for k in range(STEPS):
        own = basis[k][0:rows, :]
        out_ref[k] = own
        value = value - means[k : k + 1, :] * own
    out_ref[STEPS] = value * inverse


def shards(
    owned_blocks,
    live_count,
    row_block,
    column_block,
    send_list,
    receive_list,
    block_values,
    node_shift,
    start_vector,
):
    rows, width = start_vector.shape
    slots = block_values.shape[0]
    groups = lax.axis_size("grp")
    devices = groups * lax.axis_size("row")
    scale = 1.0 / float(devices * rows * width)
    f32 = jnp.float32

    def exchange(payload):
        parts = [payload]
        for k in range(groups - 1, 0, -1):
            if groups & (groups - 1):
                pairs = [(i, (i + k) % groups) for i in range(groups)]
            else:
                pairs = [(i, i ^ k) for i in range(groups)]
            parts.insert(1, lax.ppermute(payload, "grp", pairs))
        return parts

    def spread_out(spread):
        rows_out = lax.all_to_all(
            spread.reshape(devices, 1, LANES), AXES, split_axis=0, concat_axis=0, tiled=True
        )
        return rows_out.reshape(devices, LANES)

    spread_shape = jax.ShapeDtypeStruct((devices, LANES), f32)
    rows_scratch = pltpu.VMEM((24, LANES), f32)
    payload, index = call(
        init_kernel,
        [
            pltpu.VMEM((rows + 8, width), f32),
            pltpu.VMEM((2, slots), jnp.int32),
        ],
        [
            start_vector,
            owned_blocks.reshape(1, rows),
            row_block.reshape(1, slots),
            column_block.reshape(1, slots),
            live_count.reshape(1, 1),
        ],
        [HBM] * 5,
        [
            pltpu.VMEM((rows, width), f32),
            pltpu.VMEM((1, rows), jnp.int32),
            pltpu.VMEM((1, slots), jnp.int32),
            pltpu.VMEM((1, slots), jnp.int32),
            pltpu.VMEM((1, 1), jnp.int32),
            pltpu.SemaphoreType.DMA((5,)),
        ],
        limit=FULL - (128 << 10),
    )
    parts = exchange(payload)
    blocks, spread = call(
        setup_kernel,
        [pltpu.VMEM(block_values.shape, block_values.dtype), spread_shape],
        [block_values, payload],
        [HBM, VMEM],
        [
            pltpu.VMEM(block_values.shape, block_values.dtype),
            rows_scratch,
            pltpu.SemaphoreType.DMA((6,)),
        ],
        flops=1 << 20,
        limit=FULL - 2 * block_values.size - (1 << 20),
    )
    gathered = spread_out(spread)

    diagonal = node_shift
    tri = jnp.zeros((8, LANES), f32)
    basis = []
    for j in range(STEPS):
        outs = [
            jax.ShapeDtypeStruct((groups * rows, width), f32),
            jax.ShapeDtypeStruct((rows, width), f32),
            spread_shape,
            jax.ShapeDtypeStruct((8, LANES), f32),
        ]
        if j == 0:
            outs.append(jax.ShapeDtypeStruct((rows, width), f32))
            outs.append(jax.ShapeDtypeStruct((2, slots), jnp.int32))
        result = call(
            functools.partial(step_kernel, j, groups, scale),
            outs,
            [*parts, gathered, *basis, blocks, index, diagonal, tri],
            None,
            [
                pltpu.VMEM((width // LANES, (rows + 1) * 8, LANES), f32),
                rows_scratch,
                pltpu.SMEM((2, slots), jnp.int32),
                pltpu.SemaphoreType.DMA,
            ],
            flops=2 * slots * width * width * 8,
        )
        if j == 0:
            diagonal, index = result[4:]
        basis.append(result[0])
        image, spread, tri = result[1:4]
        gathered = spread_out(spread)
        if j < STEPS - 1:
            parts = exchange(image)
    return call(
        functools.partial(finish_kernel, scale),
        [
            jax.ShapeDtypeStruct((STEPS + 1, rows, width), f32),
            jax.ShapeDtypeStruct((2, STEPS), f32),
        ],
        [image, gathered, *basis, tri],
    )


def solution(mesh):
    return jax.shard_map(
        shards,
        mesh=mesh,
        in_specs=(
            P(("grp", "row")),
            P(("grp", "row")),
            P(("grp", "row")),
            P(("grp", "row")),
            P("grp", "row", None, None),
            P("grp", "row", None, None),
            P(("grp", "row"), None, None),
            P(("grp", "row"), None),
            P(("grp", "row"), None),
        ),
        out_specs=(P(None, ("grp", "row"), None), P()),
        check_vma=False,
    )
```

```python
import functools

import jax
import jax.numpy as jnp
from jax import lax
from jax.experimental import pallas as pl
from jax.experimental.pallas import tpu as pltpu
from jax.sharding import PartitionSpec as P

STEPS = 16
SQUARE = STEPS
NEXT = 24
CROSS = NEXT + STEPS
GRAM = 48
SUMS = 96
LANES = 128
FULL = 67_000_000 // 1024 * 1024
AXES = ("grp", "row")
VMEM = pltpu.MemorySpace.VMEM
HBM = pltpu.MemorySpace.HBM


def spec(space=VMEM):
    return pl.BlockSpec(memory_space=space)


def call(kernel, outs, operands, spaces=None, scratch=(), flops=0, limit=24 << 20):
    many = isinstance(outs, (tuple, list))
    return pl.pallas_call(
        kernel,
        out_shape=outs,
        in_specs=[spec(s) for s in (spaces or [VMEM] * len(operands))],
        out_specs=[spec()] * len(outs) if many else spec(),
        scratch_shapes=list(scratch),
        compiler_params=pltpu.CompilerParams(vmem_limit_bytes=limit),
        cost_estimate=pl.CostEstimate(flops=flops, bytes_accessed=1 << 16, transcendentals=0),
    )(*operands)


def fold(x):
    half = x.shape[1] // 2
    x = x[:, :half] + x[:, half:]
    total = x[0:8]
    for i in range(8, x.shape[0], 8):
        total = total + x[i : i + 8]
    return jnp.sum(total, axis=0, keepdims=True)


def emit_partials(rows_ref, out_ref):
    total = jnp.sum(rows_ref[...], axis=1, keepdims=True)
    place = lax.broadcasted_iota(jnp.int32, rows_ref.shape, 0)
    lane = lax.broadcasted_iota(jnp.int32, rows_ref.shape, 1)
    row = jnp.sum(jnp.where(lane == place, total, 0.0), axis=0, keepdims=True)
    out_ref[...] = jnp.broadcast_to(row, out_ref.shape)


def read_sums(gathered_ref, scale):
    total = jnp.sum(gathered_ref[...], axis=0, keepdims=True) * scale
    place = lax.broadcasted_iota(jnp.int32, (SUMS, LANES), 0)
    lane = lax.broadcasted_iota(jnp.int32, (SUMS, LANES), 1)
    return jnp.sum(jnp.where(lane == place, total, 0.0), axis=1, keepdims=True)


def column_of(row, count):
    place = lax.broadcasted_iota(jnp.int32, (count, row.shape[1]), 0)
    lane = lax.broadcasted_iota(jnp.int32, (count, row.shape[1]), 1)
    return jnp.sum(jnp.where(place == lane, row, 0), axis=1, keepdims=True)


def place_of(wanted, known, offset):
    place = lax.broadcasted_iota(jnp.int32, (known.shape[0], wanted.shape[1]), 0) + offset
    return jnp.sum(jnp.where(known == wanted, place, 0), axis=0, keepdims=True)


def init_kernel(
    start_hbm, ids_hbm, wanted_hbm, column_hbm, live_hbm, out_ref, index_ref,
    start_ref, ids_ref, wanted_ref, column_ref, live_ref, sems,
):
    pairs = [
        (start_hbm, start_ref),
        (ids_hbm, ids_ref),
        (wanted_hbm, wanted_ref),
        (column_hbm, column_ref),
        (live_hbm, live_ref),
    ]
    copies = [pltpu.make_async_copy(x, y, sems.at[i]) for i, (x, y) in enumerate(pairs)]
    for copy in copies:
        copy.start()
    for copy in copies:
        copy.wait()
    rows, width = start_ref.shape
    start = start_ref[...]
    ids = ids_ref[...]
    out_ref[0:rows, :] = start
    out_ref[rows : rows + 8, :] = jnp.zeros((8, width), jnp.float32)
    out_ref[rows : rows + 1, 0:rows] = ids.astype(jnp.float32)
    found = place_of(wanted_ref[...], column_of(ids, rows), 0)
    lane = lax.broadcasted_iota(jnp.int32, found.shape, 1)
    target = jnp.where(lane < live_ref[...], found, rows)
    index_ref[...] = jnp.concatenate([column_ref[...], target], axis=0)


def find_columns(parts, wanted):
    rows = parts[0].shape[0] - 8
    column = jnp.zeros(wanted.shape, jnp.int32)
    for p, part in enumerate(parts):
        ids = part[rows : rows + 1, 0:rows].astype(jnp.int32)
        column = column + place_of(wanted, column_of(ids, rows), rows * p)
    return column


def setup_kernel(source_hbm, payload_ref, out_ref, spread_ref, buffer_ref, rows_ref, sems):
    slots = source_hbm.shape[0]
    chunk = -(-slots // sems.shape[0])
    chunks = [pl.ds(s, min(chunk, slots - s)) for s in range(0, slots, chunk)]
    copies = [
        pltpu.make_async_copy(source_hbm.at[part], buffer_ref.at[part], sems.at[i])
        for i, part in enumerate(chunks)
    ]
    for copy in copies:
        copy.start()
    start = payload_ref[0 : payload_ref.shape[0] - 8, :]
    rows_ref[...] = jnp.zeros_like(rows_ref)
    rows_ref[SQUARE : SQUARE + 1, :] = fold(start * start)
    emit_partials(rows_ref, spread_ref)
    for part, copy in zip(chunks, copies):
        copy.wait()
        for s in range(part.start, part.start + part.size):
            out_ref[s] = buffer_ref[s].T


def tall(x):
    return jnp.broadcast_to(x, (x.shape[0], LANES))


def whole(x):
    return jnp.sum(x, axis=0, keepdims=True)


def combine(parts, basis, weights, inverse, vector_ref):
    rows = parts[0].shape[0]
    for p, part in enumerate(parts):
        value = part[...]
        for k, vector in enumerate(basis):
            value = value - weights[k : k + 1, 0:1] * vector[rows * p : rows * (p + 1), :]
        vector_ref[rows * p : rows * (p + 1), :] = value * inverse


def apply_blocks(source, left_of, blocks_ref, table_ref, acc_ref):
    halves, width = acc_ref.shape[0], blocks_ref.shape[1]
    acc_ref[...] = jnp.zeros_like(acc_ref)
    for s in range(blocks_ref.shape[0]):
        vector = jnp.broadcast_to(source(table_ref[0, s]), (8, width))
        product = jnp.dot(left_of(vector), blocks_ref[s], preferred_element_type=jnp.float32)
        target = pl.ds(pl.multiple_of(table_ref[1, s] * 8, 8), 8)
        for h in range(halves):
            acc_ref[h, target, :] = acc_ref[h, target, :] + product[:, LANES * h : LANES * (h + 1)]


def rows_of(acc_ref, i, rows):
    found = [acc_ref.at[h][pl.ds(i, rows, stride=8), :] for h in range(acc_ref.shape[0])]
    return jnp.concatenate(found, axis=1)


def rounded_left(width, ones):
    sub = lax.broadcasted_iota(jnp.int32, (8, width), 0)
    fill = jnp.where(sub == 1, 1.0, 0.0) if ones else jnp.zeros((8, width), jnp.float32)
    return lambda vector: jnp.where(sub == 0, vector, fill).astype(jnp.bfloat16)


def split_left(width):
    sub = lax.broadcasted_iota(jnp.int32, (8, width), 0)
    zero = jnp.zeros((8, width), jnp.float32)

    def left(vector):
        high = vector.astype(jnp.bfloat16).astype(jnp.float32)
        low = jnp.where(sub == 1, vector - high, zero)
        return jnp.where(sub == 0, high, low).astype(jnp.bfloat16)

    return left


def first_kernel(peers, scale, *refs):
    parts = refs[:peers]
    gathered_ref, blocks_ref, given_ref, shift_ref = refs[peers : peers + 4]
    vector_ref, out_ref, diag_ref, index_ref, acc_ref, table_ref, sem = refs[peers + 4 :]
    rows, width = shift_ref.shape
    given = given_ref[...]
    index_ref[...] = jnp.concatenate([find_columns(parts, given[0:1]), given[1:2]], axis=0)
    table = pltpu.make_async_copy(index_ref, table_ref, sem)
    table.start()
    means = read_sums(gathered_ref, scale)
    inverse = lax.rsqrt(means[SQUARE : SQUARE + 1, :] + 1e-6)
    combine([part.at[0:rows] for part in parts], [], means, inverse, vector_ref)
    table.wait()
    source = lambda i: vector_ref[pl.ds(i, 1), :]
    apply_blocks(source, rounded_left(width, True), blocks_ref, table_ref, acc_ref)
    diagonal = shift_ref[...] + rows_of(acc_ref, 1, rows)
    diag_ref[...] = diagonal
    out_ref[...] = diagonal * vector_ref[0:rows, :] - rows_of(acc_ref, 0, rows)


def look_kernel(j, peers, *refs):
    parts = refs[:peers]
    basis = refs[peers : peers + j + 1]
    blocks_ref, index_ref, diag_ref = refs[peers + j + 1 : peers + j + 4]
    spread_ref, all_ref, acc_ref, rows_ref, table_ref, sem = refs[peers + j + 4 :]
    table = pltpu.make_async_copy(index_ref, table_ref, sem)
    table.start()
    rows, width = diag_ref.shape
    for p in range(peers):
        all_ref[rows * p : rows * (p + 1), :] = parts[p][...]
    image = parts[0][...]
    rows_ref[...] = jnp.zeros_like(rows_ref)
    for k in range(j + 1):
        rows_ref[k : k + 1, :] = fold(basis[k][0:rows, :] * image)
    rows_ref[SQUARE : SQUARE + 1, :] = fold(image * image)
    for n in range(max(j - 1, 0), j + 1):
        own = basis[n][0:rows, :]
        for k in range(n + 1):
            i = GRAM + 24 * (j - n) + k
            rows_ref[i : i + 1, :] = fold(basis[k][0:rows, :] * own)
    table.wait()
    source = lambda i: all_ref[pl.ds(i, 1), :]
    apply_blocks(source, split_left(width), blocks_ref, table_ref, acc_ref)
    second = diag_ref[...] * image - (rows_of(acc_ref, 0, rows) + rows_of(acc_ref, 1, rows))
    for k in range(j + 1):
        rows_ref[NEXT + k : NEXT + k + 1, :] = fold(basis[k][0:rows, :] * second)
    rows_ref[CROSS : CROSS + 1, :] = fold(image * second)
    rows_ref[CROSS + 1 : CROSS + 2, :] = fold(second * second)
    emit_partials(rows_ref, spread_ref)


def gram_times(gram, x):
    place = lax.broadcasted_iota(jnp.int32, x.shape, 0)
    total = jnp.zeros_like(x)
    for n, upper in enumerate(gram):
        below = whole(jnp.where(place < n, upper, 0.0) * x)
        total = total + x[n : n + 1] * upper + jnp.where(place == n, below, 0.0)
    return total


def solve(j, gathered_ref, columns, gram, scale):
    means = tall(read_sums(gathered_ref, scale))
    place = lax.broadcasted_iota(jnp.int32, (24, LANES), 0)
    now = jnp.where(place <= j, means[0:24], 0.0)
    square = means[SQUARE : SQUARE + 1]
    after = jnp.where(place <= j, means[NEXT : NEXT + 24], 0.0)
    cross, second = means[CROSS : CROSS + 1], means[CROSS + 1 : CROSS + 2]
    fresh = [
        jnp.where(place <= n, means[GRAM + 24 * (j - n) : GRAM + 24 * (j - n) + 24], 0.0)
        for n in range(max(j - 1, 0), j + 1)
    ]
    gram = [g[...] for g in gram] + fresh
    gram_now = gram_times(gram, now)
    rest = jnp.maximum(square + whole(now * (gram_now - 2.0 * now)), 0.0)
    inverse = lax.rsqrt(rest + 1e-6)
    column = now + jnp.where(place == j + 1, (rest + 1e-6) * inverse, 0.0)
    mixed = jnp.zeros((24, LANES), jnp.float32)
    for m in range(j):
        mixed = mixed + now[m : m + 1] * columns[m][...]
    gram_mixed = gram_times(gram, mixed)
    last = now[j : j + 1]
    ahead = (after - gram_mixed - last * now) * inverse
    along = whole(mixed * now)
    overlap = (cross - along - last * square) * inverse
    final = (overlap - whole(now * ahead)) * inverse
    norm = second + whole(mixed * (gram_mixed - 2.0 * after))
    norm = norm + last * (last * square - 2.0 * cross + 2.0 * along)
    link = jnp.where(place <= j, now - gram_now, 0.0) * inverse
    rest_next = norm * inverse * inverse + whole(ahead * (gram_times(gram, ahead) - 2.0 * ahead))
    rest_next = rest_next + final * (2.0 * whole(link * ahead) + final * (rest * inverse * inverse - 2.0))
    rest_next = jnp.maximum(rest_next, 0.0)
    ahead = ahead + jnp.where(place == j + 1, final, 0.0)
    inverse_next = lax.rsqrt(rest_next + 1e-6)
    column_next = ahead + jnp.where(place == j + 2, (rest_next + 1e-6) * inverse_next, 0.0)
    here = (now, rest, inverse, column)
    return here, (ahead, rest_next, inverse_next, column_next), fresh


def record(tri, step, coefficient, rest):
    lane = lax.broadcasted_iota(jnp.int32, tri.shape, 1)
    place = lax.broadcasted_iota(jnp.int32, tri.shape, 0)
    column = jnp.where(place == 0, coefficient[step : step + 1], jnp.sqrt(rest))
    return jnp.where(lane == step, column, tri)


def odd_kernel(j, peers, scale, *refs):
    parts = refs[:peers]
    gathered_ref = refs[peers]
    basis = refs[peers + 1 : peers + j + 2]
    columns = refs[peers + j + 2 : peers + 2 * j + 2]
    held = max(j - 1, 0)
    gram = refs[peers + 2 * j + 2 : peers + 2 * j + 2 + held]
    blocks_ref, index_ref, diag_ref, tri_ref, *outs = refs[peers + 2 * j + 2 + held :]
    vector_ref, out_ref, next_ref, column_ref, column_next_ref, tri_out = outs[:6]
    acc_ref, table_ref, sem = outs[-3:]
    table = pltpu.make_async_copy(index_ref, table_ref, sem)
    table.start()
    rows, width = diag_ref.shape
    here, ahead, fresh = solve(j, gathered_ref, columns, gram, scale)
    for out, value in zip(outs[6:-3], fresh):
        out[...] = value
    column_ref[...] = here[3]
    column_next_ref[...] = ahead[3]
    next_ref[0:24, :] = ahead[0]
    next_ref[24:32, :] = jnp.broadcast_to(ahead[2], (8, LANES))
    tri_out[...] = record(record(tri_ref[...], j, here[0], here[1]), j + 1, ahead[0], ahead[1])
    combine(parts, basis, here[0], here[2][:, 0:1], vector_ref)
    table.wait()
    source = lambda i: vector_ref[pl.ds(i, 1), :]
    apply_blocks(source, rounded_left(width, False), blocks_ref, table_ref, acc_ref)
    out_ref[...] = diag_ref[...] * vector_ref[0:rows, :] - rows_of(acc_ref, 0, rows)


def even_kernel(j, peers, *refs):
    parts = refs[:peers]
    next_ref = refs[peers]
    basis = refs[peers + 1 : peers + j + 1]
    blocks_ref, index_ref, diag_ref = refs[peers + j + 1 : peers + j + 4]
    vector_ref, out_ref, acc_ref, table_ref, sem = refs[peers + j + 4 :]
    table = pltpu.make_async_copy(index_ref, table_ref, sem)
    table.start()
    rows, width = diag_ref.shape
    combine(parts, basis, next_ref, next_ref[24:25, 0:1], vector_ref)
    table.wait()
    source = lambda i: vector_ref[pl.ds(i, 1), :]
    apply_blocks(source, rounded_left(width, False), blocks_ref, table_ref, acc_ref)
    out_ref[...] = diag_ref[...] * vector_ref[0:rows, :] - rows_of(acc_ref, 0, rows)


def finish_kernel(image_ref, next_ref, *refs):
    basis = refs[:STEPS]
    tri_ref, out_ref, tri_out = refs[STEPS:]
    rows = image_ref.shape[0]
    tri_out[...] = tri_ref[0:2, 0:STEPS]
    value = image_ref[...]
    for k in range(STEPS):
        own = basis[k][0:rows, :]
        out_ref[k] = own
        value = value - next_ref[k : k + 1, 0:1] * own
    out_ref[STEPS] = value * next_ref[24:25, 0:1]


def shards(
    owned_blocks,
    live_count,
    row_block,
    column_block,
    send_list,
    receive_list,
    block_values,
    node_shift,
    start_vector,
):
    rows, width = start_vector.shape
    slots = block_values.shape[0]
    groups = lax.axis_size("grp")
    devices = groups * lax.axis_size("row")
    scale = 1.0 / float(devices * rows * width)
    f32 = jnp.float32

    def exchange(payload):
        parts = [payload]
        for k in range(groups - 1, 0, -1):
            if groups & (groups - 1):
                pairs = [(i, (i + k) % groups) for i in range(groups)]
            else:
                pairs = [(i, i ^ k) for i in range(groups)]
            parts.insert(1, lax.ppermute(payload, "grp", pairs))
        return parts

    def spread_out(spread):
        rows_out = lax.all_to_all(
            spread.reshape(devices, 1, LANES), AXES, split_axis=0, concat_axis=0, tiled=True
        )
        return rows_out.reshape(devices, LANES)

    spread_shape = jax.ShapeDtypeStruct((devices, LANES), f32)
    rows_scratch = pltpu.VMEM((SUMS, LANES), f32)
    payload, index = call(
        init_kernel,
        [
            pltpu.VMEM((rows + 8, width), f32),
            pltpu.VMEM((2, slots), jnp.int32),
        ],
        [
            start_vector,
            owned_blocks.reshape(1, rows),
            row_block.reshape(1, slots),
            column_block.reshape(1, slots),
            live_count.reshape(1, 1),
        ],
        [HBM] * 5,
        [
            pltpu.VMEM((rows, width), f32),
            pltpu.VMEM((1, rows), jnp.int32),
            pltpu.VMEM((1, slots), jnp.int32),
            pltpu.VMEM((1, slots), jnp.int32),
            pltpu.VMEM((1, 1), jnp.int32),
            pltpu.SemaphoreType.DMA((5,)),
        ],
        limit=FULL - (128 << 10),
    )
    parts = exchange(payload)
    blocks, spread = call(
        setup_kernel,
        [pltpu.VMEM(block_values.shape, block_values.dtype), spread_shape],
        [block_values, payload],
        [HBM, VMEM],
        [
            pltpu.VMEM(block_values.shape, block_values.dtype),
            rows_scratch,
            pltpu.SemaphoreType.DMA((6,)),
        ],
        flops=1 << 20,
        limit=FULL - 2 * block_values.size - (1 << 20),
    )
    gathered = spread_out(spread)

    vector_shape = jax.ShapeDtypeStruct((groups * rows, width), f32)
    image_shape = jax.ShapeDtypeStruct((rows, width), f32)
    small = jax.ShapeDtypeStruct((24, LANES), f32)
    acc = pltpu.VMEM((width // LANES, (rows + 1) * 8, LANES), f32)
    lookup = [pltpu.SMEM((2, slots), jnp.int32), pltpu.SemaphoreType.DMA]
    flops = 2 * slots * width * width * 8
    vector, image, diagonal, index = call(
        functools.partial(first_kernel, groups, scale),
        [vector_shape, image_shape, image_shape, jax.ShapeDtypeStruct((2, slots), jnp.int32)],
        [*parts, gathered, blocks, index, node_shift],
        None,
        [acc, *lookup],
        flops=flops,
    )
    tri = jnp.zeros((8, LANES), f32)
    basis, columns, gram = [vector], [], []
    for j in range(0, STEPS, 2):
        parts = exchange(image)
        spread = call(
            functools.partial(look_kernel, j, groups),
            spread_shape,
            [*parts, *basis, blocks, index, diagonal],
            None,
            [pltpu.VMEM((groups * rows, width), f32), acc, rows_scratch, *lookup],
            flops=flops,
        )
        gathered = spread_out(spread)
        vector, image, ahead, column, column_next, tri, *fresh = call(
            functools.partial(odd_kernel, j, groups, scale),
            [
                vector_shape,
                image_shape,
                jax.ShapeDtypeStruct((32, LANES), f32),
                small,
                small,
                jax.ShapeDtypeStruct((8, LANES), f32),
                *[small] * min(j + 1, 2),
            ],
            [*parts, gathered, *basis, *columns, *gram, blocks, index, diagonal, tri],
            None,
            [acc, *lookup],
            flops=flops,
        )
        basis.append(vector)
        columns += [column, column_next]
        gram += fresh
        if j + 2 < STEPS:
            parts = exchange(image)
            vector, image = call(
                functools.partial(even_kernel, j + 2, groups),
                [vector_shape, image_shape],
                [*parts, ahead, *basis, blocks, index, diagonal],
                None,
                [acc, *lookup],
                flops=flops,
            )
            basis.append(vector)
    return call(
        finish_kernel,
        [
            jax.ShapeDtypeStruct((STEPS + 1, rows, width), f32),
            jax.ShapeDtypeStruct((2, STEPS), f32),
        ],
        [image, ahead, *basis, tri],
    )


def solution(mesh):
    return jax.shard_map(
        shards,
        mesh=mesh,
        in_specs=(
            P(("grp", "row")),
            P(("grp", "row")),
            P(("grp", "row")),
            P(("grp", "row")),
            P("grp", "row", None, None),
            P("grp", "row", None, None),
            P(("grp", "row"), None, None),
            P(("grp", "row"), None),
            P(("grp", "row"), None),
        ),
        out_specs=(P(None, ("grp", "row"), None), P()),
        check_vma=False,
    )
```

```python
import functools

import jax
import jax.numpy as jnp
from jax import lax
from jax.experimental import pallas as pl
from jax.experimental.pallas import tpu as pltpu
from jax.sharding import PartitionSpec as P

STEPS = 16
SQUARE = STEPS
NEXT = 24
CROSS = NEXT + STEPS
GRAM = 48
SUMS = 96
LANES = 128
FULL = 67_000_000 // 1024 * 1024
AXES = ("grp", "row")
VMEM = pltpu.MemorySpace.VMEM
HBM = pltpu.MemorySpace.HBM


def spec(space=VMEM):
    return pl.BlockSpec(memory_space=space)


def call(kernel, outs, operands, spaces=None, scratch=(), flops=0, limit=24 << 20):
    many = isinstance(outs, (tuple, list))
    return pl.pallas_call(
        kernel,
        out_shape=outs,
        in_specs=[spec(s) for s in (spaces or [VMEM] * len(operands))],
        out_specs=[spec()] * len(outs) if many else spec(),
        scratch_shapes=list(scratch),
        compiler_params=pltpu.CompilerParams(vmem_limit_bytes=limit),
        cost_estimate=pl.CostEstimate(flops=flops, bytes_accessed=1 << 16, transcendentals=0),
    )(*operands)


def fold(x):
    half = x.shape[1] // 2
    x = x[:, :half] + x[:, half:]
    total = x[0:8]
    for i in range(8, x.shape[0], 8):
        total = total + x[i : i + 8]
    return jnp.sum(total, axis=0, keepdims=True)


def emit_partials(rows_ref, out_ref):
    total = jnp.sum(rows_ref[...], axis=1, keepdims=True)
    place = lax.broadcasted_iota(jnp.int32, rows_ref.shape, 0)
    lane = lax.broadcasted_iota(jnp.int32, rows_ref.shape, 1)
    row = jnp.sum(jnp.where(lane == place, total, 0.0), axis=0, keepdims=True)
    out_ref[...] = jnp.broadcast_to(row, out_ref.shape)


def read_sums(gathered_ref, scale):
    total = jnp.sum(gathered_ref[...], axis=0, keepdims=True) * scale
    place = lax.broadcasted_iota(jnp.int32, (SUMS, LANES), 0)
    lane = lax.broadcasted_iota(jnp.int32, (SUMS, LANES), 1)
    return jnp.sum(jnp.where(lane == place, total, 0.0), axis=1, keepdims=True)


def column_of(row, count):
    place = lax.broadcasted_iota(jnp.int32, (count, row.shape[1]), 0)
    lane = lax.broadcasted_iota(jnp.int32, (count, row.shape[1]), 1)
    return jnp.sum(jnp.where(place == lane, row, 0), axis=1, keepdims=True)


def place_of(wanted, known, offset):
    place = lax.broadcasted_iota(jnp.int32, (known.shape[0], wanted.shape[1]), 0) + offset
    return jnp.sum(jnp.where(known == wanted, place, 0), axis=0, keepdims=True)


def init_kernel(
    start_hbm, ids_hbm, wanted_hbm, column_hbm, live_hbm, out_ref, index_ref,
    start_ref, ids_ref, wanted_ref, column_ref, live_ref, sems,
):
    pairs = [
        (start_hbm, start_ref),
        (ids_hbm, ids_ref),
        (wanted_hbm, wanted_ref),
        (column_hbm, column_ref),
        (live_hbm, live_ref),
    ]
    copies = [pltpu.make_async_copy(x, y, sems.at[i]) for i, (x, y) in enumerate(pairs)]
    for copy in copies:
        copy.start()
    for copy in copies:
        copy.wait()
    rows, width = start_ref.shape
    start = start_ref[...]
    ids = ids_ref[...]
    out_ref[0:rows, :] = start
    out_ref[rows : rows + 8, :] = jnp.zeros((8, width), jnp.float32)
    out_ref[rows : rows + 1, 0:rows] = ids.astype(jnp.float32)
    found = place_of(wanted_ref[...], column_of(ids, rows), 0)
    lane = lax.broadcasted_iota(jnp.int32, found.shape, 1)
    target = jnp.where(lane < live_ref[...], found, rows)
    index_ref[...] = jnp.concatenate([column_ref[...], target], axis=0)


def find_columns(parts, wanted):
    rows = parts[0].shape[0] - 8
    column = jnp.zeros(wanted.shape, jnp.int32)
    for p, part in enumerate(parts):
        ids = part[rows : rows + 1, 0:rows].astype(jnp.int32)
        column = column + place_of(wanted, column_of(ids, rows), rows * p)
    return column


def setup_kernel(source_hbm, payload_ref, out_ref, spread_ref, buffer_ref, rows_ref, sems):
    slots = source_hbm.shape[0]
    chunk = -(-slots // sems.shape[0])
    chunks = [pl.ds(s, min(chunk, slots - s)) for s in range(0, slots, chunk)]
    copies = [
        pltpu.make_async_copy(source_hbm.at[part], buffer_ref.at[part], sems.at[i])
        for i, part in enumerate(chunks)
    ]
    for copy in copies:
        copy.start()
    start = payload_ref[0 : payload_ref.shape[0] - 8, :]
    rows_ref[...] = jnp.zeros_like(rows_ref)
    rows_ref[SQUARE : SQUARE + 1, :] = fold(start * start)
    emit_partials(rows_ref, spread_ref)
    for part, copy in zip(chunks, copies):
        copy.wait()
        for s in range(part.start, part.start + part.size):
            out_ref[s] = buffer_ref[s].T


def tall(x):
    return jnp.broadcast_to(x, (x.shape[0], LANES))


def whole(x):
    return jnp.sum(x, axis=0, keepdims=True)


def combine(parts, basis, weights, inverse, vector_ref):
    rows = parts[0].shape[0]
    for p, part in enumerate(parts):
        value = part[...]
        for k, vector in enumerate(basis):
            value = value - weights[k : k + 1, 0:1] * vector[rows * p : rows * (p + 1), :]
        vector_ref[rows * p : rows * (p + 1), :] = value * inverse


def entry(index_ref, i):
    return index_ref[i : i + 1, 0:1][0, 0]


def apply_blocks(source, left_of, blocks_ref, index_ref, acc_ref):
    halves, width = acc_ref.shape[0], blocks_ref.shape[1]
    acc_ref[...] = jnp.zeros_like(acc_ref)
    slots = blocks_ref.shape[0]
    for s in range(slots):
        vector = jnp.broadcast_to(source(entry(index_ref, s)), (8, width))
        product = jnp.dot(left_of(vector), blocks_ref[s], preferred_element_type=jnp.float32)
        target = pl.ds(pl.multiple_of(entry(index_ref, slots + s) * 8, 8), 8)
        for h in range(halves):
            acc_ref[h, target, :] = acc_ref[h, target, :] + product[:, LANES * h : LANES * (h + 1)]


def rows_of(acc_ref, i, rows):
    found = [acc_ref.at[h][pl.ds(i, rows, stride=8), :] for h in range(acc_ref.shape[0])]
    return jnp.concatenate(found, axis=1)


def rounded_left(width, ones):
    sub = lax.broadcasted_iota(jnp.int32, (8, width), 0)
    fill = jnp.where(sub == 1, 1.0, 0.0) if ones else jnp.zeros((8, width), jnp.float32)
    return lambda vector: jnp.where(sub == 0, vector, fill).astype(jnp.bfloat16)


def split_left(width):
    sub = lax.broadcasted_iota(jnp.int32, (8, width), 0)
    zero = jnp.zeros((8, width), jnp.float32)

    def left(vector):
        high = vector.astype(jnp.bfloat16).astype(jnp.float32)
        low = jnp.where(sub == 1, vector - high, zero)
        return jnp.where(sub == 0, high, low).astype(jnp.bfloat16)

    return left


def first_kernel(peers, scale, *refs):
    parts = refs[:peers]
    gathered_ref, blocks_ref, given_ref, shift_ref = refs[peers : peers + 4]
    vector_ref, out_ref, diag_ref, index_ref, acc_ref = refs[peers + 4 :]
    rows, width = shift_ref.shape
    given = given_ref[...]
    slots = blocks_ref.shape[0]
    for i, row in enumerate((find_columns(parts, given[0:1]), given[1:2])):
        index_ref[slots * i : slots * (i + 1), :] = tall(column_of(row, slots))
    means = read_sums(gathered_ref, scale)
    inverse = lax.rsqrt(means[SQUARE : SQUARE + 1, :] + 1e-6)
    combine([part.at[0:rows] for part in parts], [], means, inverse, vector_ref)
    source = lambda i: vector_ref[pl.ds(i, 1), :]
    apply_blocks(source, rounded_left(width, True), blocks_ref, index_ref, acc_ref)
    diagonal = shift_ref[...] + rows_of(acc_ref, 1, rows)
    diag_ref[...] = diagonal
    out_ref[...] = diagonal * vector_ref[0:rows, :] - rows_of(acc_ref, 0, rows)


def look_kernel(j, peers, *refs):
    parts = refs[:peers]
    basis = refs[peers : peers + j + 1]
    blocks_ref, index_ref, diag_ref = refs[peers + j + 1 : peers + j + 4]
    spread_ref, all_ref, acc_ref, rows_ref = refs[peers + j + 4 :]
    rows, width = diag_ref.shape
    for p in range(peers):
        all_ref[rows * p : rows * (p + 1), :] = parts[p][...]
    image = parts[0][...]
    rows_ref[...] = jnp.zeros_like(rows_ref)
    for k in range(j + 1):
        rows_ref[k : k + 1, :] = fold(basis[k][0:rows, :] * image)
    rows_ref[SQUARE : SQUARE + 1, :] = fold(image * image)
    for n in range(max(j - 1, 0), j + 1):
        own = basis[n][0:rows, :]
        for k in range(n + 1):
            i = GRAM + 24 * (j - n) + k
            rows_ref[i : i + 1, :] = fold(basis[k][0:rows, :] * own)
    source = lambda i: all_ref[pl.ds(i, 1), :]
    apply_blocks(source, split_left(width), blocks_ref, index_ref, acc_ref)
    second = diag_ref[...] * image - (rows_of(acc_ref, 0, rows) + rows_of(acc_ref, 1, rows))
    for k in range(j + 1):
        rows_ref[NEXT + k : NEXT + k + 1, :] = fold(basis[k][0:rows, :] * second)
    rows_ref[CROSS : CROSS + 1, :] = fold(image * second)
    rows_ref[CROSS + 1 : CROSS + 2, :] = fold(second * second)
    emit_partials(rows_ref, spread_ref)


def gram_times(gram, x):
    place = lax.broadcasted_iota(jnp.int32, x.shape, 0)
    total = jnp.zeros_like(x)
    for n, upper in enumerate(gram):
        below = whole(jnp.where(place < n, upper, 0.0) * x)
        total = total + x[n : n + 1] * upper + jnp.where(place == n, below, 0.0)
    return total


def solve(j, gathered_ref, columns, gram, scale):
    means = tall(read_sums(gathered_ref, scale))
    place = lax.broadcasted_iota(jnp.int32, (24, LANES), 0)
    now = jnp.where(place <= j, means[0:24], 0.0)
    square = means[SQUARE : SQUARE + 1]
    after = jnp.where(place <= j, means[NEXT : NEXT + 24], 0.0)
    cross, second = means[CROSS : CROSS + 1], means[CROSS + 1 : CROSS + 2]
    fresh = [
        jnp.where(place <= n, means[GRAM + 24 * (j - n) : GRAM + 24 * (j - n) + 24], 0.0)
        for n in range(max(j - 1, 0), j + 1)
    ]
    gram = [g[...] for g in gram] + fresh
    gram_now = gram_times(gram, now)
    rest = jnp.maximum(square + whole(now * (gram_now - 2.0 * now)), 0.0)
    inverse = lax.rsqrt(rest + 1e-6)
    column = now + jnp.where(place == j + 1, (rest + 1e-6) * inverse, 0.0)
    mixed = jnp.zeros((24, LANES), jnp.float32)
    for m in range(j):
        mixed = mixed + now[m : m + 1] * columns[m][...]
    gram_mixed = gram_times(gram, mixed)
    last = now[j : j + 1]
    ahead = (after - gram_mixed - last * now) * inverse
    along = whole(mixed * now)
    overlap = (cross - along - last * square) * inverse
    final = (overlap - whole(now * ahead)) * inverse
    norm = second + whole(mixed * (gram_mixed - 2.0 * after))
    norm = norm + last * (last * square - 2.0 * cross + 2.0 * along)
    link = jnp.where(place <= j, now - gram_now, 0.0) * inverse
    rest_next = norm * inverse * inverse + whole(ahead * (gram_times(gram, ahead) - 2.0 * ahead))
    rest_next = rest_next + final * (2.0 * whole(link * ahead) + final * (rest * inverse * inverse - 2.0))
    rest_next = jnp.maximum(rest_next, 0.0)
    ahead = ahead + jnp.where(place == j + 1, final, 0.0)
    inverse_next = lax.rsqrt(rest_next + 1e-6)
    column_next = ahead + jnp.where(place == j + 2, (rest_next + 1e-6) * inverse_next, 0.0)
    here = (now, rest, inverse, column)
    return here, (ahead, rest_next, inverse_next, column_next), fresh


def record(tri, step, coefficient, rest):
    lane = lax.broadcasted_iota(jnp.int32, tri.shape, 1)
    place = lax.broadcasted_iota(jnp.int32, tri.shape, 0)
    column = jnp.where(place == 0, coefficient[step : step + 1], jnp.sqrt(rest))
    return jnp.where(lane == step, column, tri)


def odd_kernel(j, peers, scale, *refs):
    parts = refs[:peers]
    gathered_ref = refs[peers]
    basis = refs[peers + 1 : peers + j + 2]
    columns = refs[peers + j + 2 : peers + 2 * j + 2]
    held = max(j - 1, 0)
    gram = refs[peers + 2 * j + 2 : peers + 2 * j + 2 + held]
    blocks_ref, index_ref, diag_ref, tri_ref, *outs = refs[peers + 2 * j + 2 + held :]
    vector_ref, out_ref, next_ref, column_ref, column_next_ref, tri_out = outs[:6]
    acc_ref = outs[-1]
    rows, width = diag_ref.shape
    here, ahead, fresh = solve(j, gathered_ref, columns, gram, scale)
    for out, value in zip(outs[6:-1], fresh):
        out[...] = value
    column_ref[...] = here[3]
    column_next_ref[...] = ahead[3]
    next_ref[0:24, :] = ahead[0]
    next_ref[24:32, :] = jnp.broadcast_to(ahead[2], (8, LANES))
    tri_out[...] = record(record(tri_ref[...], j, here[0], here[1]), j + 1, ahead[0], ahead[1])
    combine(parts, basis, here[0], here[2][:, 0:1], vector_ref)
    source = lambda i: vector_ref[pl.ds(i, 1), :]
    apply_blocks(source, rounded_left(width, False), blocks_ref, index_ref, acc_ref)
    out_ref[...] = diag_ref[...] * vector_ref[0:rows, :] - rows_of(acc_ref, 0, rows)


def even_kernel(j, peers, *refs):
    parts = refs[:peers]
    next_ref = refs[peers]
    basis = refs[peers + 1 : peers + j + 1]
    blocks_ref, index_ref, diag_ref = refs[peers + j + 1 : peers + j + 4]
    vector_ref, out_ref, acc_ref = refs[peers + j + 4 :]
    rows, width = diag_ref.shape
    combine(parts, basis, next_ref, next_ref[24:25, 0:1], vector_ref)
    source = lambda i: vector_ref[pl.ds(i, 1), :]
    apply_blocks(source, rounded_left(width, False), blocks_ref, index_ref, acc_ref)
    out_ref[...] = diag_ref[...] * vector_ref[0:rows, :] - rows_of(acc_ref, 0, rows)


def finish_kernel(image_ref, next_ref, *refs):
    basis = refs[:STEPS]
    tri_ref, out_ref, tri_out = refs[STEPS:]
    rows = image_ref.shape[0]
    tri_out[...] = tri_ref[0:2, 0:STEPS]
    value = image_ref[...]
    for k in range(STEPS):
        own = basis[k][0:rows, :]
        out_ref[k] = own
        value = value - next_ref[k : k + 1, 0:1] * own
    out_ref[STEPS] = value * next_ref[24:25, 0:1]


def shards(
    owned_blocks,
    live_count,
    row_block,
    column_block,
    send_list,
    receive_list,
    block_values,
    node_shift,
    start_vector,
):
    rows, width = start_vector.shape
    slots = block_values.shape[0]
    groups = lax.axis_size("grp")
    devices = groups * lax.axis_size("row")
    scale = 1.0 / float(devices * rows * width)
    f32 = jnp.float32

    def exchange(payload):
        parts = [payload]
        for k in range(groups - 1, 0, -1):
            if groups & (groups - 1):
                pairs = [(i, (i + k) % groups) for i in range(groups)]
            else:
                pairs = [(i, i ^ k) for i in range(groups)]
            parts.insert(1, lax.ppermute(payload, "grp", pairs))
        return parts

    def spread_out(spread):
        rows_out = lax.all_to_all(
            spread.reshape(devices, 1, LANES), AXES, split_axis=0, concat_axis=0, tiled=True
        )
        return rows_out.reshape(devices, LANES)

    spread_shape = jax.ShapeDtypeStruct((devices, LANES), f32)
    rows_scratch = pltpu.VMEM((SUMS, LANES), f32)
    payload, index = call(
        init_kernel,
        [
            pltpu.VMEM((rows + 8, width), f32),
            pltpu.VMEM((2, slots), jnp.int32),
        ],
        [
            start_vector,
            owned_blocks.reshape(1, rows),
            row_block.reshape(1, slots),
            column_block.reshape(1, slots),
            live_count.reshape(1, 1),
        ],
        [HBM] * 5,
        [
            pltpu.VMEM((rows, width), f32),
            pltpu.VMEM((1, rows), jnp.int32),
            pltpu.VMEM((1, slots), jnp.int32),
            pltpu.VMEM((1, slots), jnp.int32),
            pltpu.VMEM((1, 1), jnp.int32),
            pltpu.SemaphoreType.DMA((5,)),
        ],
        limit=FULL - (128 << 10),
    )
    parts = exchange(payload)
    blocks, spread = call(
        setup_kernel,
        [pltpu.VMEM(block_values.shape, block_values.dtype), spread_shape],
        [block_values, payload],
        [HBM, VMEM],
        [
            pltpu.VMEM(block_values.shape, block_values.dtype),
            rows_scratch,
            pltpu.SemaphoreType.DMA((6,)),
        ],
        flops=1 << 20,
        limit=FULL - 2 * block_values.size - (3 << 20),
    )
    gathered = spread_out(spread)

    vector_shape = jax.ShapeDtypeStruct((groups * rows, width), f32)
    image_shape = jax.ShapeDtypeStruct((rows, width), f32)
    small = jax.ShapeDtypeStruct((24, LANES), f32)
    acc = pltpu.VMEM((width // LANES, (rows + 1) * 8, LANES), f32)
    flops = 2 * slots * width * width * 8
    vector, image, diagonal, index = call(
        functools.partial(first_kernel, groups, scale),
        [vector_shape, image_shape, image_shape, jax.ShapeDtypeStruct((2 * slots, LANES), jnp.int32)],
        [*parts, gathered, blocks, index, node_shift],
        None,
        [acc],
        flops=flops,
    )
    tri = jnp.zeros((8, LANES), f32)
    basis, columns, gram = [vector], [], []
    for j in range(0, STEPS, 2):
        parts = exchange(image)
        spread = call(
            functools.partial(look_kernel, j, groups),
            spread_shape,
            [*parts, *basis, blocks, index, diagonal],
            None,
            [pltpu.VMEM((groups * rows, width), f32), acc, rows_scratch],
            flops=flops,
        )
        gathered = spread_out(spread)
        vector, image, ahead, column, column_next, tri, *fresh = call(
            functools.partial(odd_kernel, j, groups, scale),
            [
                vector_shape,
                image_shape,
                jax.ShapeDtypeStruct((32, LANES), f32),
                small,
                small,
                jax.ShapeDtypeStruct((8, LANES), f32),
                *[small] * min(j + 1, 2),
            ],
            [*parts, gathered, *basis, *columns, *gram, blocks, index, diagonal, tri],
            None,
            [acc],
            flops=flops,
        )
        basis.append(vector)
        columns += [column, column_next]
        gram += fresh
        if j + 2 < STEPS:
            parts = exchange(image)
            vector, image = call(
                functools.partial(even_kernel, j + 2, groups),
                [vector_shape, image_shape],
                [*parts, ahead, *basis, blocks, index, diagonal],
                None,
                [acc],
                flops=flops,
            )
            basis.append(vector)
    return call(
        finish_kernel,
        [
            jax.ShapeDtypeStruct((STEPS + 1, rows, width), f32),
            jax.ShapeDtypeStruct((2, STEPS), f32),
        ],
        [image, ahead, *basis, tri],
    )


def solution(mesh):
    return jax.shard_map(
        shards,
        mesh=mesh,
        in_specs=(
            P(("grp", "row")),
            P(("grp", "row")),
            P(("grp", "row")),
            P(("grp", "row")),
            P("grp", "row", None, None),
            P("grp", "row", None, None),
            P(("grp", "row"), None, None),
            P(("grp", "row"), None),
            P(("grp", "row"), None),
        ),
        out_specs=(P(None, ("grp", "row"), None), P()),
        check_vma=False,
    )
```
